32 devices in a mesh: batch: 8 (over z, x), cols: 4 (over y, core).
Axes of the slice: x: 2, y: 2, z: 4, core: 2. Of those that a mesh axis runs over, the one named last changes fastest.
Arguments:
- partial_query: float32 [8, 1024, 1024], P('batch', None, 'cols'), may hold values from -0.875 to 0.875
- partial_key: float32 [8, 1024, 1024], P('batch', None, 'cols'), may hold values from -0.875 to 0.875
- partial_value: float32 [8, 1024, 1024], P('batch', None, 'cols'), may hold values from -0.875 to 0.875
- partial_mixed: float32 [8, 1024, 1024], P('batch', 'cols'), may hold values from -0.875 to 0.875
- partial_norm: float32 [8, 1024], P('batch'), may hold values from -8 to 8
- partial_bias: float32 [8, 1024], P('batch'), may hold values from -8 to 8
- master_query: float32 [1024, 1024], P('batch', 'cols'), may hold values from -0.1875 to 0.1875
- master_key: float32 [1024, 1024], P('batch', 'cols'), may hold values from -0.1875 to 0.1875
- master_value: float32 [1024, 1024], P('batch', 'cols'), may hold values from -0.1875 to 0.1875
- master_mixed: float32 [1024, 1024], P('cols', 'batch'), may hold values from -0.1875 to 0.1875
- master_norm: float32 [1024], P('batch'), may hold values from 0.25 to 1.75
- master_bias: float32 [1024], P('batch'), may hold values from -3 to 3
Outputs:
- compute_query: bfloat16 [1024, 1024], P(None, 'cols')
- compute_key: bfloat16 [1024, 1024], P(None, 'cols')
- compute_value: bfloat16 [1024, 1024], P(None, 'cols')
- compute_mixed: bfloat16 [1024, 1024], P('cols')
- compute_norm: bfloat16 [1024], replicated
- compute_bias: bfloat16 [1024], replicated
- stepped_query: float32 [1024, 1024], P('batch', 'cols')
- stepped_key: float32 [1024, 1024], P('batch', 'cols')
- stepped_value: float32 [1024, 1024], P('batch', 'cols')
- stepped_mixed: float32 [1024, 1024], P('cols', 'batch')
- stepped_norm: float32 [1024], P('batch')
- stepped_bias: float32 [1024], P('batch')
The draws below stay inside these ranges and needn't reach their ends.
All inputs are finite; a program needn't handle non-finite values.
Results may differ from the reference program's by a relative error of at most 0.001.
Values may be sent and summed in bfloat16 or wider, within the bound.
No kernel may reach another device: no remote copies, remote signals or barrier semaphores. Data moves between devices by JAX's collectives and lax.ppermute only.
A program may use at most 64 MiB of HBM per device.

```python
import jax
import jax.numpy as jnp

WIDTH = 1024
ATTN = 1024
REPLICAS = 8


def with_spikes(array, stream_key, source, target, blocks, factor):
    owner, partner = [(jnp.arange(array.shape[axis_at]) // (array.shape[axis_at] // blocks)).reshape([-1 if axis == axis_at else 1 for axis in range(array.ndim)]) for axis_at in (source, target)]
    chosen = jax.random.permutation(stream_key, blocks)[partner]
    strong = (owner == chosen) | (owner == (partner + blocks // 2) % blocks)
    return jnp.where(strong, factor * array, array)


def levels(rng, extent, cuts, smallest, top_value):
    def one(position, blocks):
        heights = jax.random.uniform(jax.random.fold_in(jax.random.fold_in(rng, 6), position), (blocks,), jnp.float32, smallest / len(cuts), top_value / len(cuts))
        return jnp.repeat(jnp.exp(heights), extent[position] // blocks).reshape((-1,) + (1,) * (len(extent) - position - 1))

    loudness = one(*cuts[0])
    for cut in cuts[1:]:
        loudness = loudness * one(*cut)
    return loudness


def gaussian(stream_key, extent, spread, limit, shards=(), dtype=jnp.bfloat16):
    loudness = levels(stream_key, extent, shards, -0.22, 0.18) if shards else 1.0
    drawn = jax.random.normal(stream_key, extent, jnp.float32) * spread * loudness
    return jnp.minimum(jnp.maximum(drawn, -limit), limit).astype(dtype)


def heavy_noise(stream_key, dims, deviation, reach, cuts, heavy, kind=jnp.bfloat16):
    drawn = deviation * jax.random.normal(stream_key, dims, jnp.float32)
    if cuts:
        drawn = drawn * levels(stream_key, dims, cuts, -0.22, 0.18)
    return jnp.clip(with_spikes(drawn, jax.random.fold_in(stream_key, 3), *heavy), -reach, reach).astype(kind)


def setup_inputs(seed: int = 0) -> dict:
    splits = jax.random.split(jax.random.key(seed), 13)
    partial_query = heavy_noise(splits[0], (REPLICAS, WIDTH, ATTN), 0.1, 0.875, ((0, 8), (2, 4)), (0, 1, 8, 2.0), jnp.float32)
    partial_key = heavy_noise(splits[1], (REPLICAS, WIDTH, ATTN), 0.1, 0.875, ((0, 8), (2, 4)), (0, 1, 8, 2.0), jnp.float32)
    partial_value = heavy_noise(splits[2], (REPLICAS, WIDTH, ATTN), 0.1, 0.875, ((0, 8), (2, 4)), (0, 1, 8, 2.0), jnp.float32)
    partial_mixed = heavy_noise(splits[3], (REPLICAS, ATTN, WIDTH), 0.1, 0.875, ((0, 8), (1, 4)), (0, 2, 8, 2.0), jnp.float32)
    partial_norm = heavy_noise(splits[4], (REPLICAS, WIDTH), 1.0, 8.0, ((0, 8),), (0, 1, 8, 2.0), jnp.float32)
    partial_bias = heavy_noise(splits[5], (REPLICAS, WIDTH), 1.0, 8.0, ((0, 8),), (0, 1, 8, 2.0), jnp.float32)
    master_query = gaussian(splits[6], (WIDTH, ATTN), WIDTH ** -0.5, 0.1875, ((0, 8), (1, 4)), jnp.float32)
    master_key = gaussian(splits[7], (WIDTH, ATTN), WIDTH ** -0.5, 0.1875, ((0, 8), (1, 4)), jnp.float32)
    master_value = gaussian(splits[8], (WIDTH, ATTN), WIDTH ** -0.5, 0.1875, ((0, 8), (1, 4)), jnp.float32)
    master_mixed = gaussian(splits[9], (ATTN, WIDTH), ATTN ** -0.5, 0.1875, ((0, 4), (1, 8)), jnp.float32)
    master_norm = jnp.clip(1.0 + 0.15 * jax.random.normal(splits[10], (WIDTH,), jnp.float32), 0.25, 1.75)
    master_bias = gaussian(splits[11], (WIDTH,), 0.5, 3.0, ((0, 8),), jnp.float32)
    return {"partial_query": partial_query, "partial_key": partial_key, "partial_value": partial_value, "partial_mixed": partial_mixed, "partial_norm": partial_norm, "partial_bias": partial_bias, "master_query": master_query, "master_key": master_key, "master_value": master_value, "master_mixed": master_mixed, "master_norm": master_norm, "master_bias": master_bias}


learn_rate = 0.4


def reference(partial_query, partial_key, partial_value, partial_mixed, partial_norm, partial_bias, master_query, master_key, master_value, master_mixed, master_norm, master_bias):
    mean_query = jnp.sum(partial_query.astype(jnp.float32), axis=0) * REPLICAS ** -0.5
    mean_key = jnp.sum(partial_key.astype(jnp.float32), axis=0) * REPLICAS ** -0.5
    mean_value = jnp.sum(partial_value.astype(jnp.float32), axis=0) * REPLICAS ** -0.5
    mean_mixed = jnp.sum(partial_mixed.astype(jnp.float32), axis=0) * REPLICAS ** -0.5
    mean_norm = jnp.sum(partial_norm.astype(jnp.float32), axis=0) * REPLICAS ** -0.5
    mean_bias = jnp.sum(partial_bias.astype(jnp.float32), axis=0) * REPLICAS ** -0.5
    stepped_query = master_query - learn_rate * mean_query
    stepped_key = master_key - learn_rate * mean_key
    stepped_value = master_value - learn_rate * mean_value
    stepped_mixed = master_mixed - learn_rate * mean_mixed
    stepped_norm = master_norm - learn_rate * mean_norm
    stepped_bias = master_bias - learn_rate * mean_bias
    compute_query = stepped_query.astype(jnp.bfloat16)
    compute_key = stepped_key.astype(jnp.bfloat16)
    compute_value = stepped_value.astype(jnp.bfloat16)
    compute_mixed = stepped_mixed.astype(jnp.bfloat16)
    compute_norm = stepped_norm.astype(jnp.bfloat16)
    compute_bias = stepped_bias.astype(jnp.bfloat16)
    return compute_query, compute_key, compute_value, compute_mixed, compute_norm, compute_bias, stepped_query, stepped_key, stepped_value, stepped_mixed, stepped_norm, stepped_bias
```

```python
import math

import jax
import jax.numpy as jnp
from jax import lax
from jax.experimental import pallas as pl
from jax.experimental.pallas import tpu as pltpu
from jax.sharding import PartitionSpec as P

learn_rate = 0.4
lanes = 128
tail_rows = 16
vmem_grant = 16 << 20
largest_partial = 12.0


def sizes_of(query, mixed, replicas):
    rows, cols = query.shape[0] // replicas, query.shape[1]
    fits = (
        rows % lanes == 0
        and cols == 2 * rows
        and mixed.shape == (cols, rows * replicas)
    )
    return rows, cols, fits


def split(x):
    wide = x * 8193.0
    high = wide - (wide - x)
    return high, x - high


def own_lines(line, here, height):
    high, low = split(line)
    row = lax.broadcasted_iota(jnp.int32, (height, line.shape[-1]), 0)
    return jnp.where(row == 2 * here, high, 0.0) + jnp.where(row == 2 * here + 1, low, 0.0)


def pack_plain(arrays, chunks, replicas, here):
    query, key, value, mixed, norm, bias = arrays
    rows, cols, _ = sizes_of(query, mixed, replicas)
    out = []
    for at in chunks:
        parts = [lax.dynamic_slice_in_dim(a, at * rows, rows, 0) for a in (query, key, value)]
        parts.append(lax.dynamic_slice_in_dim(mixed, at * rows, rows, 1).reshape(rows, cols))
        pair = [lax.dynamic_slice_in_dim(a, at * rows, rows, 0) for a in (norm, bias)]
        line = jnp.pad(jnp.concatenate(pair), (0, cols - 2 * rows))[None]
        if here is not None:
            line = own_lines(line, here, 2 * replicas)
        out.append(jnp.concatenate(parts + [line]))
    return out


def pack_tiles(arrays, offsets, replicas, name):
    query, key, value, mixed, norm, bias = arrays
    rows, cols, _ = sizes_of(query, mixed, replicas)
    height = 4 * rows + 2 * replicas

    def kernel(q, k, v, m, n, b, out, sems):
        here = lax.axis_index("batch")
        started = []
        for j, offset in enumerate(offsets):
            start = pl.multiple_of((here ^ offset) * rows, lanes)
            copies = []
            for i, ref in enumerate((q, k, v)):
                copies.append((ref.at[pl.ds(start, rows), :], out.at[j, pl.ds(i * rows, rows), :]))
            for i in range(2):
                copies.append(
                    (
                        m.at[pl.ds(i * rows, rows), pl.ds(start, rows)],
                        out.at[j, pl.ds(3 * rows, rows), pl.ds(i * rows, rows)],
                    )
                )
            started += [pltpu.make_async_copy(*c, sems.at[j]) for c in copies]
        for c in started:
            c.start()
        for j, offset in enumerate(offsets):
            start = pl.multiple_of((here ^ offset) * rows, lanes)
            for i, ref in enumerate((n, b)):
                lines = own_lines(ref[:, pl.ds(start, rows)], here, 2 * replicas)
                out[j, pl.ds(4 * rows, 2 * replicas), pl.ds(i * rows, rows)] = lines
        for c in started:
            c.wait()

    hbm = pl.BlockSpec(memory_space=pltpu.HBM)
    vmem = pl.BlockSpec(memory_space=pltpu.VMEM)
    slabs = pl.pallas_call(
        kernel,
        out_shape=jax.ShapeDtypeStruct((len(offsets), height, cols), jnp.float32),
        in_specs=[hbm] * 4 + [vmem] * 2,
        out_specs=vmem,
        scratch_shapes=[pltpu.SemaphoreType.DMA((len(offsets),))],
        name=name,
        compiler_params=pltpu.CompilerParams(vmem_limit_bytes=vmem_grant),
    )(query, key, value, mixed, norm[None], bias[None])
    return [slabs[j] for j in range(len(offsets))]


def step_plain(total, masters, rate, rows, cols):
    own = [masters[i] - rate * total[i * rows : (i + 1) * rows] for i in range(3)]
    own.append(masters[3] - rate * total[3 * rows : 4 * rows].reshape(cols, rows))
    line = jnp.sum(total[4 * rows :], axis=0)
    own += [masters[4] - rate * line[:rows], masters[5] - rate * line[rows : 2 * rows]]
    line = jnp.pad(jnp.concatenate(own[4:]), (0, cols - 2 * rows))[None]
    slab = own[:3] + [own[3].reshape(rows, cols), jnp.broadcast_to(line, (tail_rows, cols))]
    return (jnp.concatenate([x.astype(jnp.bfloat16) for x in slab]), *own)


def step_tiles(total, masters, rate, rows, cols):
    def kernel(total, q, k, v, m, n, b, slab, sq, sk, sv, sm, sn, sb):
        for i, (old, new) in enumerate(((q, sq), (k, sk), (v, sv))):
            at = pl.ds(i * rows, rows)
            new[...] = old[...] - rate * total[at, :]
            slab[at, :] = new[...].astype(jnp.bfloat16)
        for i in range(2):
            at, half = pl.ds(3 * rows, rows), pl.ds(i * rows, rows)
            sm[half, :] = m[half, :] - rate * total[at, half]
            slab[at, half] = sm[half, :].astype(jnp.bfloat16)
        line = jnp.sum(total[pl.ds(4 * rows, total.shape[0] - 4 * rows), :], axis=0, keepdims=True)
        for i, (old, new) in enumerate(((n, sn), (b, sb))):
            half = slice(i * rows, (i + 1) * rows)
            new[...] = old[...] - rate * line[:, half]
            tail = jnp.broadcast_to(new[...], (tail_rows, rows)).astype(jnp.bfloat16)
            slab[pl.ds(4 * rows, tail_rows), half] = tail

    masters = (*masters[:4], masters[4][None], masters[5][None])
    vmem = pl.BlockSpec(memory_space=pltpu.VMEM)
    slab, *own = pl.pallas_call(
        kernel,
        out_shape=[jax.ShapeDtypeStruct((4 * rows + tail_rows, cols), jnp.bfloat16)]
        + [jax.ShapeDtypeStruct(x.shape, jnp.float32) for x in masters],
        in_specs=[vmem] * 7,
        out_specs=[vmem] * 7,
        name="step",
        compiler_params=pltpu.CompilerParams(vmem_limit_bytes=vmem_grant),
    )(total, *masters)
    return (slab, *own[:4], own[4].reshape(-1), own[5].reshape(-1))


def unpack_tiles(pieces, rows, cols, replicas):
    def kernel(*refs):
        got = refs[:replicas]
        q, k, v, m, n, b, nf, bf, sem = refs[replicas:]
        here = lax.axis_index("batch")
        started = []
        for j, piece in enumerate(got):
            at = here ^ j
            start = pl.multiple_of(at * rows, lanes)
            for i, ref in enumerate((q, k, v)):
                started.append(pltpu.make_async_copy(piece.at[pl.ds(i * rows, rows), :], ref.at[pl.ds(start, rows), :], sem.at[0]))
            for i in range(2):
                started.append(
                    pltpu.make_async_copy(
                        piece.at[pl.ds(3 * rows, rows), pl.ds(i * rows, rows)],
                        m.at[pl.ds(i * rows, rows), pl.ds(start, rows)],
                        sem.at[0],
                    )
                )
        for c in started:
            c.start()
        for j, piece in enumerate(got):
            line = piece[pl.ds(4 * rows, tail_rows), :].astype(jnp.float32)
            nf[pl.ds(here ^ j, 1), :] = line[0:1, :rows]
            bf[pl.ds(here ^ j, 1), :] = line[0:1, rows:]
        n[...] = nf[...].astype(jnp.bfloat16)
        b[...] = bf[...].astype(jnp.bfloat16)
        for c in started:
            c.wait()

    tall = jax.ShapeDtypeStruct((replicas * rows, cols), jnp.bfloat16)
    wide = jax.ShapeDtypeStruct((cols, replicas * rows), jnp.bfloat16)
    line = jax.ShapeDtypeStruct((replicas, rows), jnp.bfloat16)
    hbm = pl.BlockSpec(memory_space=pltpu.HBM)
    vmem = pl.BlockSpec(memory_space=pltpu.VMEM)
    *full, norm, bias = pl.pallas_call(
        kernel,
        out_shape=[tall, tall, tall, wide, line, line],
        in_specs=[vmem] * replicas,
        out_specs=[hbm] * 4 + [vmem] * 2,
        scratch_shapes=[
            pltpu.VMEM((replicas, rows), jnp.float32),
            pltpu.VMEM((replicas, rows), jnp.float32),
            pltpu.SemaphoreType.DMA((1,)),
        ],
        name="unpack",
        compiler_params=pltpu.CompilerParams(vmem_limit_bytes=vmem_grant),
    )(*pieces)
    return (*full, norm.reshape(-1), bias.reshape(-1))


def unpack_plain(pieces, rows, cols, replicas):
    here = lax.axis_index("batch")
    stacked = jnp.stack(pieces)
    ordered = stacked[jnp.arange(replicas) ^ here]
    full = [ordered[:, i * rows : (i + 1) * rows].reshape(replicas * rows, cols) for i in range(3)]
    mixed = ordered[:, 3 * rows : 4 * rows].reshape(replicas, cols, rows)
    full.append(mixed.transpose(1, 0, 2).reshape(cols, replicas * rows))
    tail = ordered[:, 4 * rows]
    return (*full, tail[:, :rows].reshape(-1), tail[:, rows : 2 * rows].reshape(-1))


def per_device(*arrays):
    partials = tuple(a[0] for a in arrays[:6])
    masters = arrays[6:]
    replicas = lax.axis_size("batch")
    here = lax.axis_index("batch")
    rows, cols, fits = sizes_of(partials[0], partials[3], replicas)
    bits = [1 << i for i in range(replicas.bit_length() - 1)]
    scale = 2.0 ** math.floor(math.log2(65504.0 / (largest_partial * replicas)))
    away = [j for j in range(replicas - 1, 0, -1) if j & 1]
    home = [j for j in range(replicas - 2, -1, -1) if not j & 1]

    if fits:
        slabs = dict(zip(away, pack_tiles(partials, away, replicas, "pack_away")))
        slabs.update(zip(home, pack_tiles(partials, home, replicas, "pack_home")))
    else:
        slabs = dict(zip(away + home, pack_plain(partials, [here ^ j for j in away + home], replicas, here)))

    def swap(x, bit):
        return lax.ppermute(x, "batch", [(i, i ^ bit) for i in range(replicas)])

    terms = {j: [slabs[j] * scale] for j in slabs}
    for bit in bits:
        for j in [j for j in range(replicas - 1, 0, -1) if j & bit and not j & (bit - 1)]:
            got = swap(sum(terms[j]).astype(jnp.float16), bit)
            terms[j ^ bit].append(got.astype(jnp.float32))
    rate = learn_rate * replicas**-0.5 / scale
    step = step_tiles if fits else step_plain
    slab, *own = step(sum(terms[0]), masters, rate, rows, cols)

    pieces = {0: slab}
    for bit in reversed(bits):
        for j in list(pieces):
            pieces[j ^ bit] = swap(pieces[j], bit)
    pieces = [pieces[j] for j in range(replicas)]
    full = (unpack_tiles if fits else unpack_plain)(pieces, rows, cols, replicas)
    return (*full, *own)


def solution(mesh):
    in_specs = (
        P("batch", None, "cols"),
        P("batch", None, "cols"),
        P("batch", None, "cols"),
        P("batch", "cols", None),
        P("batch", None),
        P("batch", None),
        P("batch", "cols"),
        P("batch", "cols"),
        P("batch", "cols"),
        P("cols", "batch"),
        P("batch"),
        P("batch"),
    )
    out_specs = (
        P(None, "cols"),
        P(None, "cols"),
        P(None, "cols"),
        P("cols", None),
        P(),
        P(),
        P("batch", "cols"),
        P("batch", "cols"),
        P("batch", "cols"),
        P("cols", "batch"),
        P("batch"),
        P("batch"),
    )
    return jax.shard_map(
        per_device, mesh=mesh, in_specs=in_specs, out_specs=out_specs, check_vma=False
    )
```

```python
import math

import jax
import jax.numpy as jnp
from jax import lax
from jax.experimental import pallas as pl
from jax.experimental.pallas import tpu as pltpu
from jax.sharding import PartitionSpec as P


learn_rate = 0.4
lanes = 128
tail_rows = 16
vmem_grant = 16 << 20
largest_partial = 12.0


def sizes_of(query, mixed, replicas):
    rows, cols = query.shape[0] // replicas, query.shape[1]
    fits = (
        rows % lanes == 0
        and cols == 2 * rows
        and mixed.shape == (cols, rows * replicas)
    )
    return rows, cols, fits


def groups_of(fits):
    return [(0, 1), (2, 3, 4, 5)] if fits else [(0, 1, 2, 3, 4, 5)]


def split(x):
    wide = x * 8193.0
    high = wide - (wide - x)
    return high, x - high


def own_lines(line, here, height):
    high, low = split(line)
    row = lax.broadcasted_iota(jnp.int32, (height, line.shape[-1]), 0)
    return jnp.where(row == 2 * here, high, 0.0) + jnp.where(row == 2 * here + 1, low, 0.0)


def pack_plain(arrays, chunks, replicas, here):
    query, key, value, mixed, norm, bias = arrays
    rows, cols, _ = sizes_of(query, mixed, replicas)
    out = []
    for at in chunks:
        parts = [lax.dynamic_slice_in_dim(a, at * rows, rows, 0) for a in (query, key, value)]
        parts.append(lax.dynamic_slice_in_dim(mixed, at * rows, rows, 1).reshape(rows, cols))
        pair = [lax.dynamic_slice_in_dim(a, at * rows, rows, 0) for a in (norm, bias)]
        line = jnp.pad(jnp.concatenate(pair), (0, cols - 2 * rows))[None]
        if here is not None:
            line = own_lines(line, here, 2 * replicas)
        out.append(jnp.concatenate(parts + [line]))
    return out


def pack_tiles(arrays, offsets, replicas):
    query, key, value, mixed, norm, bias = arrays
    rows, cols, _ = sizes_of(query, mixed, replicas)
    height = 4 * rows + 2 * replicas

    def kernel(q, k, v, m, n, b, out, lines, sems, line_sem):
        here = lax.axis_index("batch")
        vectors = [pltpu.make_async_copy(ref, lines.at[pl.ds(i, 1)], line_sem.at[0]) for i, ref in enumerate((n, b))]
        for c in vectors:
            c.start()
        started = []
        for j, offset in enumerate(offsets):
            start = pl.multiple_of((here ^ offset) * rows, lanes)
            copies = []
            for i, ref in enumerate((q, k, v)):
                copies.append((ref.at[pl.ds(start, rows), :], out.at[j, pl.ds(i * rows, rows), :]))
            for i in range(2):
                copies.append(
                    (
                        m.at[pl.ds(i * rows, rows), pl.ds(start, rows)],
                        out.at[j, pl.ds(3 * rows, rows), pl.ds(i * rows, rows)],
                    )
                )
            started += [pltpu.make_async_copy(*c, sems.at[j]) for c in copies]
        for c in started:
            c.start()
        for c in vectors:
            c.wait()
        for j, offset in enumerate(offsets):
            start = pl.multiple_of((here ^ offset) * rows, lanes)
            for i in range(2):
                own = own_lines(lines[pl.ds(i, 1), pl.ds(start, rows)], here, 2 * replicas)
                out[j, pl.ds(4 * rows, 2 * replicas), pl.ds(i * rows, rows)] = own
        for c in started:
            c.wait()

    partials = (query, key, value, mixed, norm[None], bias[None])
    slabs = pl.pallas_call(
        kernel,
        out_shape=jax.ShapeDtypeStruct((len(offsets), height, cols), jnp.float32),
        in_specs=[pl.BlockSpec(memory_space=pltpu.HBM)] * 6,
        out_specs=pl.BlockSpec(memory_space=pltpu.VMEM),
        scratch_shapes=[
            pltpu.VMEM((2, rows * replicas), jnp.float32),
            pltpu.SemaphoreType.DMA((len(offsets),)),
            pltpu.SemaphoreType.DMA((1,)),
        ],
        compiler_params=pltpu.CompilerParams(vmem_limit_bytes=vmem_grant),
    )(*[pltpu.with_memory_space_constraint(x, pltpu.HBM) for x in partials])
    return [slabs[j] for j in range(len(offsets))]


def step_plain(total, masters, parts, rate, rows, cols):
    own = [masters[i] - rate * total[i * rows : (i + 1) * rows] for i in range(3)]
    own.append(masters[3] - rate * total[3 * rows : 4 * rows].reshape(cols, rows))
    line = jnp.sum(total[4 * rows :], axis=0)
    own += [masters[4] - rate * line[:rows], masters[5] - rate * line[rows : 2 * rows]]
    line = jnp.pad(jnp.concatenate(own[4:]), (0, cols - 2 * rows))[None]
    slab = own[:3] + [own[3].reshape(rows, cols), jnp.broadcast_to(line, (tail_rows, cols))]
    return jnp.concatenate([x.astype(jnp.bfloat16) for x in slab]), own


def step_tiles(total, masters, parts, rate, rows, cols):
    masters = [masters[p] if p < 4 else masters[p][None] for p in parts]
    height = rows * sum(p < 4 for p in parts)
    tail = tail_rows if 4 in parts else 0

    def kernel(total, *refs):
        olds, slab, news = refs[: len(parts)], refs[len(parts)], refs[len(parts) + 1 :]
        if tail:
            line = jnp.sum(total[pl.ds(height, total.shape[0] - height), :], axis=0, keepdims=True)
        for i, (p, old, new) in enumerate(zip(parts, olds, news)):
            if p < 3:
                at = pl.ds(i * rows, rows)
                new[...] = old[...] - rate * total[at, :]
                slab[at, :] = new[...].astype(jnp.bfloat16)
            elif p == 3:
                for h in range(2):
                    at, half = pl.ds(i * rows, rows), pl.ds(h * rows, rows)
                    new[half, :] = old[half, :] - rate * total[at, half]
                    slab[at, half] = new[half, :].astype(jnp.bfloat16)
            else:
                half = slice((p - 4) * rows, (p - 3) * rows)
                new[...] = old[...] - rate * line[:, half]
                ends = jnp.broadcast_to(new[...], (tail, rows)).astype(jnp.bfloat16)
                slab[pl.ds(height, tail), half] = ends

    vmem = pl.BlockSpec(memory_space=pltpu.VMEM)
    slab, *own = pl.pallas_call(
        kernel,
        out_shape=[jax.ShapeDtypeStruct((height + tail, cols), jnp.bfloat16)]
        + [jax.ShapeDtypeStruct(x.shape, jnp.float32) for x in masters],
        in_specs=[vmem] * (1 + len(parts)),
        out_specs=[vmem] * (1 + len(parts)),
        name="step",
        compiler_params=pltpu.CompilerParams(vmem_limit_bytes=vmem_grant),
    )(total, *masters)
    return slab, [x if p < 4 else x.reshape(-1) for p, x in zip(parts, own)]


def unpack_tiles(pieces, tick, parts, rows, cols):
    replicas = len(pieces)
    height = rows * sum(p < 4 for p in parts)
    vectors = [p for p in parts if p > 3]

    def kernel(*refs):
        got, outs = refs[:replicas], refs[replicas + 1 : replicas + 1 + len(parts)]
        *lines, sem = refs[replicas + 1 + len(parts) :]
        here = lax.axis_index("batch")
        started = []
        for j, piece in enumerate(got):
            start = pl.multiple_of((here ^ j) * rows, lanes)
            for i, (p, out) in enumerate(zip(parts, outs)):
                at = pl.ds(i * rows, rows)
                if p < 3:
                    pairs = [(piece.at[at, :], out.at[pl.ds(start, rows), :])]
                elif p == 3:
                    halves = [pl.ds(h * rows, rows) for h in range(2)]
                    pairs = [(piece.at[at, half], out.at[half, pl.ds(start, rows)]) for half in halves]
                else:
                    pairs = []
                started += [pltpu.make_async_copy(*pair, sem.at[0]) for pair in pairs]
        for c in started:
            c.start()
        for j, piece in enumerate(got):
            for p, line in zip(vectors, lines):
                tail = piece[pl.ds(height, tail_rows), pl.ds((p - 4) * rows, rows)]
                line[pl.ds(here ^ j, 1), :] = tail.astype(jnp.float32)[0:1]
        for line, out in zip(lines, outs[len(parts) - len(vectors) :]):
            out[...] = line[...].astype(jnp.bfloat16)
        for c in started:
            c.wait()

    shapes = [(replicas * rows, cols)] * 3 + [(cols, replicas * rows)] + [(replicas, rows)] * 2
    hbm = pl.BlockSpec(memory_space=pltpu.HBM)
    vmem = pl.BlockSpec(memory_space=pltpu.VMEM)
    outs = pl.pallas_call(
        kernel,
        out_shape=[jax.ShapeDtypeStruct(shapes[p], jnp.bfloat16) for p in parts],
        in_specs=[vmem] * (replicas + 1),
        out_specs=[hbm if p < 4 else vmem for p in parts],
        scratch_shapes=[pltpu.VMEM((replicas, rows), jnp.float32) for _ in vectors] + [pltpu.SemaphoreType.DMA((1,))],
        name="unpack",
        compiler_params=pltpu.CompilerParams(vmem_limit_bytes=vmem_grant),
    )(*pieces, tick)
    return [x if p < 4 else x.reshape(-1) for p, x in zip(parts, outs)]


def unpack_plain(pieces, rows, cols, replicas):
    here = lax.axis_index("batch")
    stacked = jnp.stack(pieces)
    ordered = stacked[jnp.arange(replicas) ^ here]
    full = [ordered[:, i * rows : (i + 1) * rows].reshape(replicas * rows, cols) for i in range(3)]
    mixed = ordered[:, 3 * rows : 4 * rows].reshape(replicas, cols, rows)
    full.append(mixed.transpose(1, 0, 2).reshape(cols, replicas * rows))
    tail = ordered[:, 4 * rows]
    return (*full, tail[:, :rows].reshape(-1), tail[:, rows : 2 * rows].reshape(-1))


order_of_8 = (
    (0, 7, 0), (0, 7, 1), (0, 5, 0), (0, 6, 1), (0, 3, 0), (0, 6, 0), (0, 5, 1), (0, 1, 0), (0, 3, 1),
    (0, 4, 0), (0, 2, 0), (0, 4, 1), (0, 2, 1), (0, 1, 1), (1, 4, 0), (1, 1, 0), (1, 2, 0), (1, 4, 1),
    (1, 1, 1), (1, 2, 1), (1, 3, 0), (1, 5, 0), (1, 5, 1), (1, 6, 0), (1, 3, 1), (1, 6, 1), (1, 7, 0),
    (1, 7, 1),
)
bits_of_8 = {(0, 7, 1): 2, (1, 7, 0): 2}
packs_of_8 = ((7,), (6, 5, 3, 1,), (4, 2, 0,))


def plan_of(replicas, fits):
    groups = groups_of(fits)
    every = [(w, j, g) for w in range(2) for j in range(1, replicas) for g in range(len(groups))]
    bits = {at: at[1] & -at[1] for at in every}
    if fits and replicas == 8:
        bits.update(bits_of_8)
        return groups, bits, list(order_of_8)
    chunks = [*range(replicas - 1, 0, -2), *range(replicas - 2, 0, -2)]
    back = sorted(range(1, replicas), key=lambda j: (j & 1, j.bit_count(), j))
    return groups, bits, [(w, j, g) for w, order in ((0, chunks), (1, back)) for j in order for g in range(len(groups))]


def inputs_of(at, bits):
    w, j, g = at
    if w == 0:
        return [k for k in bits if k[0] == 0 and k[2] == g and k[1] ^ bits[k] == j]
    if j != bits[at]:
        return [(1, j ^ bits[at], g)]
    return [k for k in bits if k[0] == 0 and k[2] == g and k[1] == bits[k]]


def ticks_of(bits, order):
    late, seen = {}, set()
    for before, at in zip(order, order[1:]):
        new = [k for k in inputs_of(at, bits) if k not in seen]
        seen.update(new)
        if new and new != [before]:
            late[before] = [k for k in new if k != before]
    return late


def replica_step(*arrays):
    partials = tuple(a[0] for a in arrays[:6])
    masters = arrays[6:]
    replicas = lax.axis_size("batch")
    here = lax.axis_index("batch")
    rows, cols, fits = sizes_of(partials[0], partials[3], replicas)
    scale = 2.0 ** math.floor(math.log2(65504.0 / (largest_partial * replicas)))
    groups, bits, order = plan_of(replicas, fits)
    every = range(replicas)
    calls = packs_of_8 if fits and replicas == 8 else (tuple(every),)

    if fits:
        slabs = {}
        for chunks in calls:
            slabs.update(zip(chunks, pack_tiles(partials, chunks, replicas)))
    else:
        slabs = dict(zip(every, pack_plain(partials, [here ^ j for j in every], replicas, here)))

    def swap(x, bit):
        return lax.ppermute(x, "batch", [(i, i ^ bit) for i in range(replicas)])

    tall = slabs[0].shape[0]
    bounds = []
    for g, parts in enumerate(groups):
        first = rows * sum(p < 4 for q in groups[:g] for p in q)
        bounds.append((first, tall if 4 in parts else first + rows * len(parts)))
    got = {(j, g): [] for j in slabs for g in range(len(groups))}
    ahead = None

    def total(j, g):
        nonlocal ahead
        low, high = bounds[g]
        mine = slabs[j][low:high] * scale
        if not got[j, g]:
            return mine
        if ahead is not None:
            got[j, g][0], ahead = lax.optimization_barrier((got[j, g][0], ahead))
        return sum((x.astype(jnp.float32) for x in got[j, g]), mine)

    rate = learn_rate * replicas**-0.5 / scale
    ticks = ticks_of(bits, order) if fits else {}
    tick = masters[4][None]
    own, full, pieces = [None] * 6, [None] * 6, {}
    for at in order:
        w, j, g = at
        bit = bits[at]
        if w == 0:
            send = total(j, g).astype(jnp.float16)
            if got[j, g]:
                ahead = send
            got[j ^ bit, g].append(swap(send, bit))
        else:
            if (0, g) not in pieces:
                ahead = total(0, g)
                step = step_tiles if fits else step_plain
                pieces[0, g], new = step(ahead, masters, groups[g], rate, rows, cols)
                for p, x in zip(groups[g], new):
                    own[p] = x
            pieces[j, g] = swap(pieces[j ^ bit, g], bit)
        if at in ticks:
            tick = lax.optimization_barrier(tick) + 1.0
    for g, parts in enumerate(groups):
        mine = [pieces[j, g] for j in range(replicas)]
        done = unpack_tiles(mine, tick, parts, rows, cols) if fits else unpack_plain(mine, rows, cols, replicas)
        for p, x in zip(parts, done):
            full[p] = x
    return (*full, *own)


def solution(mesh):
    in_specs = (
        P("batch", None, "cols"),
        P("batch", None, "cols"),
        P("batch", None, "cols"),
        P("batch", "cols", None),
        P("batch", None),
        P("batch", None),
        P("batch", "cols"),
        P("batch", "cols"),
        P("batch", "cols"),
        P("cols", "batch"),
        P("batch"),
        P("batch"),
    )
    out_specs = (
        P(None, "cols"),
        P(None, "cols"),
        P(None, "cols"),
        P("cols", None),
        P(),
        P(),
        P("batch", "cols"),
        P("batch", "cols"),
        P("batch", "cols"),
        P("cols", "batch"),
        P("batch"),
        P("batch"),
    )
    return jax.shard_map(replica_step, mesh=mesh, in_specs=in_specs, out_specs=out_specs, check_vma=False)
```

```python
import math

import jax
import jax.numpy as jnp
from jax import lax
from jax.experimental import pallas as pl
from jax.experimental.pallas import tpu as pltpu
from jax.sharding import PartitionSpec as P


learn_rate = 0.4
lanes = 128
tail_rows = 8
vmem_grant = 16 << 20
largest_partial = 12.0


def sizes_of(query, mixed, replicas):
    rows, cols = query.shape[0] // replicas, query.shape[1]
    fits = (
        rows % lanes == 0
        and cols == 2 * rows
        and mixed.shape == (cols, rows * replicas)
    )
    return rows, cols, fits


def groups_of(fits):
    return [(0, 1), (2, 3, 4, 5)] if fits else [(0, 1, 2, 3, 4, 5)]


def split(x):
    wide = x * 8193.0
    high = wide - (wide - x)
    return high, x - high


def own_lines(line, here, height):
    high, low = split(line)
    row = lax.broadcasted_iota(jnp.int32, (height, line.shape[-1]), 0)
    return jnp.where(row == 2 * here, high, 0.0) + jnp.where(row == 2 * here + 1, low, 0.0)


def pack_plain(arrays, chunks, replicas, here):
    query, key, value, mixed, norm, bias = arrays
    rows, cols, _ = sizes_of(query, mixed, replicas)
    out = []
    for at in chunks:
        parts = [lax.dynamic_slice_in_dim(a, at * rows, rows, 0) for a in (query, key, value)]
        parts.append(lax.dynamic_slice_in_dim(mixed, at * rows, rows, 1).reshape(rows, cols))
        pair = [lax.dynamic_slice_in_dim(a, at * rows, rows, 0) for a in (norm, bias)]
        line = jnp.pad(jnp.concatenate(pair), (0, cols - 2 * rows))[None]
        if here is not None:
            line = own_lines(line, here, 2 * replicas)
        out.append(jnp.concatenate(parts + [line]))
    return out


def pack_tiles(arrays, offsets, replicas):
    query, key, value, mixed, norm, bias = arrays
    rows, cols, _ = sizes_of(query, mixed, replicas)
    height = 4 * rows + 2 * replicas

    def kernel(q, k, v, m, n, b, out, lines, sems, line_sem):
        here = lax.axis_index("batch")
        vectors = [pltpu.make_async_copy(ref, lines.at[pl.ds(i, 1)], line_sem.at[0]) for i, ref in enumerate((n, b))]
        for c in vectors:
            c.start()
        started = []
        for j, offset in enumerate(offsets):
            start = pl.multiple_of((here ^ offset) * rows, lanes)
            copies = []
            for i, ref in enumerate((q, k, v)):
                copies.append((ref.at[pl.ds(start, rows), :], out.at[j, pl.ds(i * rows, rows), :]))
            for i in range(2):
                copies.append(
                    (
                        m.at[pl.ds(i * rows, rows), pl.ds(start, rows)],
                        out.at[j, pl.ds(3 * rows, rows), pl.ds(i * rows, rows)],
                    )
                )
            started += [pltpu.make_async_copy(*c, sems.at[j]) for c in copies]
        for c in started:
            c.start()
        for c in vectors:
            c.wait()
        for j, offset in enumerate(offsets):
            start = pl.multiple_of((here ^ offset) * rows, lanes)
            for i in range(2):
                own = own_lines(lines[pl.ds(i, 1), pl.ds(start, rows)], here, 2 * replicas)
                out[j, pl.ds(4 * rows, 2 * replicas), pl.ds(i * rows, rows)] = own
        for c in started:
            c.wait()

    partials = (query, key, value, mixed, norm[None], bias[None])
    slabs = pl.pallas_call(
        kernel,
        out_shape=jax.ShapeDtypeStruct((len(offsets), height, cols), jnp.float32),
        in_specs=[pl.BlockSpec(memory_space=pltpu.HBM)] * 6,
        out_specs=pl.BlockSpec(memory_space=pltpu.VMEM),
        scratch_shapes=[
            pltpu.VMEM((2, rows * replicas), jnp.float32),
            pltpu.SemaphoreType.DMA((len(offsets),)),
            pltpu.SemaphoreType.DMA((1,)),
        ],
        compiler_params=pltpu.CompilerParams(vmem_limit_bytes=vmem_grant),
    )(*[pltpu.with_memory_space_constraint(x, pltpu.HBM) for x in partials])
    return [slabs[j] for j in range(len(offsets))]


def step_plain(total, masters, parts, rate, rows, cols):
    own = [masters[i] - rate * total[i * rows : (i + 1) * rows] for i in range(3)]
    own.append(masters[3] - rate * total[3 * rows : 4 * rows].reshape(cols, rows))
    line = jnp.sum(total[4 * rows :], axis=0)
    own += [masters[4] - rate * line[:rows], masters[5] - rate * line[rows : 2 * rows]]
    line = jnp.pad(jnp.concatenate(own[4:]), (0, cols - 2 * rows))[None]
    slab = own[:3] + [own[3].reshape(rows, cols), jnp.broadcast_to(line, (tail_rows, cols))]
    return jnp.concatenate([x.astype(jnp.bfloat16) for x in slab]), own


def step_tiles(total, masters, parts, rate, rows, cols):
    masters = [masters[p] if p < 4 else masters[p][None] for p in parts]
    height = rows * sum(p < 4 for p in parts)
    tail = tail_rows if 4 in parts else 0

    def kernel(total, *refs):
        olds, slab, news = refs[: len(parts)], refs[len(parts)], refs[len(parts) + 1 :]
        if tail:
            line = jnp.sum(total[pl.ds(height, total.shape[0] - height), :], axis=0, keepdims=True)
        for i, (p, old, new) in enumerate(zip(parts, olds, news)):
            if p < 3:
                at = pl.ds(i * rows, rows)
                new[...] = old[...] - rate * total[at, :]
                slab[at, :] = new[...].astype(jnp.bfloat16)
            elif p == 3:
                for h in range(2):
                    at, half = pl.ds(i * rows, rows), pl.ds(h * rows, rows)
                    new[half, :] = old[half, :] - rate * total[at, half]
                    slab[at, half] = new[half, :].astype(jnp.bfloat16)
            else:
                half = slice((p - 4) * rows, (p - 3) * rows)
                new[...] = old[...] - rate * line[:, half]
                ends = jnp.broadcast_to(new[...], (tail, rows)).astype(jnp.bfloat16)
                slab[pl.ds(height, tail), half] = ends

    vmem = pl.BlockSpec(memory_space=pltpu.VMEM)
    slab, *own = pl.pallas_call(
        kernel,
        out_shape=[jax.ShapeDtypeStruct((height + tail, cols), jnp.bfloat16)]
        + [jax.ShapeDtypeStruct(x.shape, jnp.float32) for x in masters],
        in_specs=[vmem] * (1 + len(parts)),
        out_specs=[vmem] * (1 + len(parts)),
        name="step",
        compiler_params=pltpu.CompilerParams(vmem_limit_bytes=vmem_grant),
    )(total, *masters)
    return slab, [x if p < 4 else x.reshape(-1) for p, x in zip(parts, own)]


def unpack_tiles(pieces, begun, tick, parts, rows, cols, replicas):
    height = rows * sum(p < 4 for p in parts)
    vectors = [p for p in parts if p > 3]
    slabs = sorted(pieces)
    ends = not begun and len(slabs) == replicas or bool(begun)
    lines_out = [(replicas, rows)] * len(vectors)

    def kernel(*refs):
        refs = list(refs)
        got = [refs.pop(0) for _ in slabs]
        refs.pop(0)
        earlier = [refs.pop(0) for _ in begun]
        outs = [refs.pop(0) for _ in parts]
        *lines, sem = refs
        started = []
        for j, piece in zip(slabs, got):
            start = pl.multiple_of((lax.axis_index("batch") ^ j) * rows, lanes)
            for i, (p, out) in enumerate(zip(parts, outs)):
                at = pl.ds(i * rows, rows)
                if p < 3:
                    pairs = [(piece.at[at, :], out.at[pl.ds(start, rows), :])]
                elif p == 3:
                    halves = [pl.ds(h * rows, rows) for h in range(2)]
                    pairs = [(piece.at[at, half], out.at[half, pl.ds(start, rows)]) for half in halves]
                else:
                    pairs = []
                started += [pltpu.make_async_copy(*pair, sem.at[0]) for pair in pairs]
        for c in started:
            c.start()
        for line, old in zip(lines, earlier[len(parts) - len(vectors) :]):
            line[...] = old[...]
        for j, piece in zip(slabs, got):
            for p, line in zip(vectors, lines):
                tail = piece[pl.ds(height, tail_rows), pl.ds((p - 4) * rows, rows)]
                line[pl.ds(lax.axis_index("batch") ^ j, 1), :] = tail.astype(jnp.float32)[0:1]
        for line, out in zip(lines, outs[len(parts) - len(vectors) :]):
            out[...] = line[...].astype(out.dtype)
        for c in started:
            c.wait()

    shapes = [(replicas * rows, cols)] * 3 + [(cols, replicas * rows)] + [(replicas, rows)] * 2
    kinds = [jnp.bfloat16 if p < 4 or ends else jnp.float32 for p in parts]
    hbm = pl.BlockSpec(memory_space=pltpu.HBM)
    vmem = pl.BlockSpec(memory_space=pltpu.VMEM)
    spaces = [hbm if p < 4 else vmem for p in parts]
    outs = pl.pallas_call(
        kernel,
        out_shape=[jax.ShapeDtypeStruct(shapes[p], kind) for p, kind in zip(parts, kinds)],
        in_specs=[vmem] * (len(slabs) + 1) + (spaces if begun else []),
        out_specs=spaces,
        scratch_shapes=[pltpu.VMEM(x, jnp.float32) for x in lines_out] + [pltpu.SemaphoreType.DMA((1,))],
        input_output_aliases={len(slabs) + 1 + i: i for i, p in enumerate(parts) if p < 4} if begun else {},
        name="unpack",
        compiler_params=pltpu.CompilerParams(vmem_limit_bytes=vmem_grant),
    )(*[pieces[j] for j in slabs], tick, *begun)
    return [x if p < 4 or not ends else x.reshape(-1) for p, x in zip(parts, outs)]


def unpack_plain(pieces, rows, cols, replicas):
    here = lax.axis_index("batch")
    stacked = jnp.stack(pieces)
    ordered = stacked[jnp.arange(replicas) ^ here]
    full = [ordered[:, i * rows : (i + 1) * rows].reshape(replicas * rows, cols) for i in range(3)]
    mixed = ordered[:, 3 * rows : 4 * rows].reshape(replicas, cols, rows)
    full.append(mixed.transpose(1, 0, 2).reshape(cols, replicas * rows))
    tail = ordered[:, 4 * rows]
    return (*full, tail[:, :rows].reshape(-1), tail[:, rows : 2 * rows].reshape(-1))


order_of_8 = (
    ((0, 7, 0),), ((0, 5, 0),), ((0, 7, 1),), ((0, 3, 0),), ((0, 6, 0),), ((0, 6, 1),), ((0, 5, 1),),
    ((0, 3, 1),), ((0, 1, 0),), ((0, 4, 0),), ((0, 2, 0),), ((0, 4, 1),), ((0, 2, 1),), ((0, 1, 1),),
    ((1, 4, 0),), ((1, 1, 0),), ((1, 2, 0),), ((1, 1, 1),), ((1, 4, 1),), ((1, 2, 1),), ((1, 3, 0),),
    ((1, 5, 0),), ((1, 5, 1),), ((1, 6, 1),), ((1, 6, 0),), ((1, 3, 1),), ((1, 7, 0),), ((1, 7, 1),),
)
bits_of_8 = {(0, 7, 1): 2, (1, 7, 0): 2}
packs_of_8 = ((7, 5, 3), (6, 1, 4, 2, 0))


def plan_of(replicas, fits):
    groups = groups_of(fits)
    every = [(w, j, g) for w in range(2) for j in range(1, replicas) for g in range(len(groups))]
    bits = {at: at[1] & -at[1] for at in every}
    if fits and replicas == 8:
        bits.update(bits_of_8)
        return groups, bits, list(order_of_8)
    chunks = [*range(replicas - 1, 0, -2), *range(replicas - 2, 0, -2)]
    back = sorted(range(1, replicas), key=lambda j: (j & 1, j.bit_count(), j))
    order = [((w, j, g),) for w, js in ((0, chunks), (1, back)) for j in js for g in range(len(groups))]
    return groups, bits, order


def inputs_of(at, bits):
    w, j, g = at
    if w == 0:
        return [k for k in bits if k[0] == 0 and k[2] == g and k[1] ^ bits[k] == j]
    if j != bits[at]:
        return [(1, j ^ bits[at], g)]
    return [k for k in bits if k[0] == 0 and k[2] == g and k[1] == bits[k]]


def ticks_of(bits, order):
    late, seen = {}, set()
    home = {at: exchange for exchange in order for at in exchange}
    for before, exchange in zip(order, order[1:]):
        new = []
        for at in exchange:
            new += [home[k] for k in inputs_of(at, bits) if home[k] not in seen and home[k] not in new]
        seen.update(new)
        new = [k for k in new if k != before]
        if new:
            late[before] = new
    return late


def replica_step(*arrays):
    partials = tuple(a[0] for a in arrays[:6])
    masters = arrays[6:]
    replicas = lax.axis_size("batch")
    here = lax.axis_index("batch")
    rows, cols, fits = sizes_of(partials[0], partials[3], replicas)
    scale = 2.0 ** math.floor(math.log2(65504.0 / (largest_partial * replicas)))
    groups, bits, order = plan_of(replicas, fits)
    every = range(replicas)
    calls = packs_of_8 if fits and replicas == 8 else (tuple(every),)

    if fits:
        slabs = {}
        for chunks in calls:
            slabs.update(zip(chunks, pack_tiles(partials, chunks, replicas)))
    else:
        slabs = dict(zip(every, pack_plain(partials, [here ^ j for j in every], replicas, here)))

    def swap(xs, exchange):
        (bit,) = {bits[at] for at in exchange}
        x = xs[0] if len(xs) == 1 else jnp.concatenate(xs)
        x = lax.ppermute(x, "batch", [(i, i ^ bit) for i in every])
        ends = [sum(y.shape[0] for y in xs[: i + 1]) for i in range(len(xs))]
        return [x] if len(xs) == 1 else [x[end - y.shape[0] : end] for end, y in zip(ends, xs)]

    tall = slabs[0].shape[0]
    bounds = []
    for g, parts in enumerate(groups):
        first = rows * sum(p < 4 for q in groups[:g] for p in q)
        bounds.append((first, tall if 4 in parts else first + rows * len(parts)))
    got = {(j, g): [] for j in slabs for g in range(len(groups))}
    ahead = None

    def total(j, g):
        nonlocal ahead
        low, high = bounds[g]
        mine = slabs[j][low:high] * scale
        if not got[j, g]:
            return mine
        if ahead is not None:
            got[j, g][0], ahead = lax.optimization_barrier((got[j, g][0], ahead))
        return sum((x.astype(jnp.float32) for x in got[j, g]), mine)

    rate = learn_rate * replicas**-0.5 / scale
    ticks = ticks_of(bits, order) if fits else {}
    tick = masters[4][None]
    own, full, pieces = [None] * 6, [None] * 6, {}
    for exchange in order:
        sends = []
        for w, j, g in exchange:
            if w == 0:
                sends.append(total(j, g).astype(jnp.float16))
                if got[j, g]:
                    ahead = sends[-1]
                continue
            if (0, g) not in pieces:
                ahead = total(0, g)
                step = step_tiles if fits else step_plain
                pieces[0, g], new = step(ahead, masters, groups[g], rate, rows, cols)
                for p, x in zip(groups[g], new):
                    own[p] = x
            sends.append(pieces[j ^ bits[w, j, g], g])
        for (w, j, g), x in zip(exchange, swap(sends, exchange)):
            if w == 0:
                got[j ^ bits[w, j, g], g].append(x)
            else:
                pieces[j, g] = x
        if exchange in ticks:
            tick = lax.optimization_barrier(tick) + 1.0
    for g, parts in enumerate(groups):
        mine = {j: pieces[j, g] for j in range(replicas)}
        if not fits:
            done = unpack_plain([mine[j] for j in range(replicas)], rows, cols, replicas)
        elif g == order[-1][-1][2]:
            last = {at[1]: mine.pop(at[1]) for at in order[-1]}
            done = unpack_tiles(mine, [], tick, parts, rows, cols, replicas)
            done = unpack_tiles(last, done, tick, parts, rows, cols, replicas)
        else:
            done = unpack_tiles(mine, [], tick, parts, rows, cols, replicas)
        for p, x in zip(parts, done):
            full[p] = x
    return (*full, *own)


def solution(mesh):
    in_specs = (
        P("batch", None, "cols"),
        P("batch", None, "cols"),
        P("batch", None, "cols"),
        P("batch", "cols", None),
        P("batch", None),
        P("batch", None),
        P("batch", "cols"),
        P("batch", "cols"),
        P("batch", "cols"),
        P("cols", "batch"),
        P("batch"),
        P("batch"),
    )
    out_specs = (
        P(None, "cols"),
        P(None, "cols"),
        P(None, "cols"),
        P("cols", None),
        P(),
        P(),
        P("batch", "cols"),
        P("batch", "cols"),
        P("batch", "cols"),
        P("cols", "batch"),
        P("batch"),
        P("batch"),
    )
    return jax.shard_map(replica_step, mesh=mesh, in_specs=in_specs, out_specs=out_specs, check_vma=False)
```

```python
import math

import jax
import jax.numpy as jnp
from jax import lax
from jax.experimental import pallas as pl
from jax.experimental.pallas import tpu as pltpu
from jax.sharding import PartitionSpec as P


learn_rate = 0.4
lanes = 128
tail_rows = 8
vmem_grant = 16 << 20
largest_partial = 12.0


def sizes_of(query, mixed, replicas):
    rows, cols = query.shape[0] // replicas, query.shape[1]
    fits = (
        rows % lanes == 0
        and cols == 2 * rows
        and mixed.shape == (cols, rows * replicas)
    )
    return rows, cols, fits


def groups_of(fits):
    return [(0, 1), (2, 3, 4, 5)] if fits else [(0, 1, 2, 3, 4, 5)]


def split(x):
    wide = x * 8193.0
    high = wide - (wide - x)
    return high, x - high


def own_lines(line, here, height):
    high, low = split(line)
    row = lax.broadcasted_iota(jnp.int32, (height, line.shape[-1]), 0)
    return jnp.where(row == 2 * here, high, 0.0) + jnp.where(row == 2 * here + 1, low, 0.0)


def pack_plain(arrays, chunks, replicas, here):
    query, key, value, mixed, norm, bias = arrays
    rows, cols, _ = sizes_of(query, mixed, replicas)
    out = []
    for at in chunks:
        parts = [lax.dynamic_slice_in_dim(a, at * rows, rows, 0) for a in (query, key, value)]
        parts.append(lax.dynamic_slice_in_dim(mixed, at * rows, rows, 1).reshape(rows, cols))
        pair = [lax.dynamic_slice_in_dim(a, at * rows, rows, 0) for a in (norm, bias)]
        line = jnp.pad(jnp.concatenate(pair), (0, cols - 2 * rows))[None]
        if here is not None:
            line = own_lines(line, here, 2 * replicas)
        out.append(jnp.concatenate(parts + [line]))
    return out


def pack_tiles(arrays, offsets, replicas):
    query, key, value, mixed, norm, bias = arrays
    rows, cols, _ = sizes_of(query, mixed, replicas)
    height = 4 * rows + 2 * replicas

    def kernel(q, k, v, m, n, b, out, lines, sems, line_sem):
        here = lax.axis_index("batch")
        vectors = [pltpu.make_async_copy(ref, lines.at[pl.ds(i, 1)], line_sem.at[0]) for i, ref in enumerate((n, b))]
        for c in vectors:
            c.start()
        started = []
        for j, offset in enumerate(offsets):
            start = pl.multiple_of((here ^ offset) * rows, lanes)
            copies = []
            for i, ref in enumerate((q, k, v)):
                copies.append((ref.at[pl.ds(start, rows), :], out.at[j, pl.ds(i * rows, rows), :]))
            for i in range(2):
                copies.append(
                    (
                        m.at[pl.ds(i * rows, rows), pl.ds(start, rows)],
                        out.at[j, pl.ds(3 * rows, rows), pl.ds(i * rows, rows)],
                    )
                )
            started += [pltpu.make_async_copy(*c, sems.at[j]) for c in copies]
        for c in started:
            c.start()
        for c in vectors:
            c.wait()
        for j, offset in enumerate(offsets):
            start = pl.multiple_of((here ^ offset) * rows, lanes)
            for i in range(2):
                own = own_lines(lines[pl.ds(i, 1), pl.ds(start, rows)], here, 2 * replicas)
                out[j, pl.ds(4 * rows, 2 * replicas), pl.ds(i * rows, rows)] = own
        for c in started:
            c.wait()

    partials = (query, key, value, mixed, norm[None], bias[None])
    slabs = pl.pallas_call(
        kernel,
        out_shape=jax.ShapeDtypeStruct((len(offsets), height, cols), jnp.float32),
        in_specs=[pl.BlockSpec(memory_space=pltpu.HBM)] * 6,
        out_specs=pl.BlockSpec(memory_space=pltpu.VMEM),
        scratch_shapes=[
            pltpu.VMEM((2, rows * replicas), jnp.float32),
            pltpu.SemaphoreType.DMA((len(offsets),)),
            pltpu.SemaphoreType.DMA((1,)),
        ],
        compiler_params=pltpu.CompilerParams(vmem_limit_bytes=vmem_grant),
    )(*[pltpu.with_memory_space_constraint(x, pltpu.HBM) for x in partials])
    return [slabs[j] for j in range(len(offsets))]


def step_plain(total, masters, parts, rate, rows, cols):
    own = [masters[i] - rate * total[i * rows : (i + 1) * rows] for i in range(3)]
    own.append(masters[3] - rate * total[3 * rows : 4 * rows].reshape(cols, rows))
    line = jnp.sum(total[4 * rows :], axis=0)
    own += [masters[4] - rate * line[:rows], masters[5] - rate * line[rows : 2 * rows]]
    line = jnp.pad(jnp.concatenate(own[4:]), (0, cols - 2 * rows))[None]
    slab = own[:3] + [own[3].reshape(rows, cols), jnp.broadcast_to(line, (tail_rows, cols))]
    return jnp.concatenate([x.astype(jnp.bfloat16) for x in slab]), own


def step_tiles(total, masters, parts, rate, rows, cols):
    masters = [masters[p] if p < 4 else masters[p][None] for p in parts]
    height = rows * sum(p < 4 for p in parts)
    tail = tail_rows if 4 in parts else 0

    def kernel(total, *refs):
        olds, slab, news = refs[: len(parts)], refs[len(parts)], refs[len(parts) + 1 :]
        if tail:
            line = jnp.sum(total[pl.ds(height, total.shape[0] - height), :], axis=0, keepdims=True)
        for i, (p, old, new) in enumerate(zip(parts, olds, news)):
            if p < 3:
                at = pl.ds(i * rows, rows)
                new[...] = old[...] - rate * total[at, :]
                slab[at, :] = new[...].astype(jnp.bfloat16)
            elif p == 3:
                for h in range(2):
                    at, half = pl.ds(i * rows, rows), pl.ds(h * rows, rows)
                    new[half, :] = old[half, :] - rate * total[at, half]
                    slab[at, half] = new[half, :].astype(jnp.bfloat16)
            else:
                half = slice((p - 4) * rows, (p - 3) * rows)
                new[...] = old[...] - rate * line[:, half]
                ends = jnp.broadcast_to(new[...], (tail, rows)).astype(jnp.bfloat16)
                slab[pl.ds(height, tail), half] = ends

    vmem = pl.BlockSpec(memory_space=pltpu.VMEM)
    slab, *own = pl.pallas_call(
        kernel,
        out_shape=[jax.ShapeDtypeStruct((height + tail, cols), jnp.bfloat16)]
        + [jax.ShapeDtypeStruct(x.shape, jnp.float32) for x in masters],
        in_specs=[vmem] * (1 + len(parts)),
        out_specs=[vmem] * (1 + len(parts)),
        name="step",
        compiler_params=pltpu.CompilerParams(vmem_limit_bytes=vmem_grant),
    )(total, *masters)
    return slab, [x if p < 4 else x.reshape(-1) for p, x in zip(parts, own)]


def unpack_tiles(pieces, begun, tick, parts, rows, cols, replicas):
    height = rows * sum(p < 4 for p in parts)
    vectors = [p for p in parts if p > 3]
    slabs = sorted(pieces)
    ends = not begun and len(slabs) == replicas or bool(begun)
    lines_out = [(replicas, rows)] * len(vectors)

    def kernel(*refs):
        refs = list(refs)
        got = [refs.pop(0) for _ in slabs]
        refs.pop(0)
        earlier = [refs.pop(0) for _ in begun]
        outs = [refs.pop(0) for _ in parts]
        *lines, sem = refs
        started = []
        for j, piece in zip(slabs, got):
            start = pl.multiple_of((lax.axis_index("batch") ^ j) * rows, lanes)
            for i, (p, out) in enumerate(zip(parts, outs)):
                at = pl.ds(i * rows, rows)
                if p < 3:
                    pairs = [(piece.at[at, :], out.at[pl.ds(start, rows), :])]
                elif p == 3:
                    halves = [pl.ds(h * rows, rows) for h in range(2)]
                    pairs = [(piece.at[at, half], out.at[half, pl.ds(start, rows)]) for half in halves]
                else:
                    pairs = []
                started += [pltpu.make_async_copy(*pair, sem.at[0]) for pair in pairs]
        for c in started:
            c.start()
        for line, old in zip(lines, earlier[len(parts) - len(vectors) :]):
            line[...] = old[...]
        for j, piece in zip(slabs, got):
            for p, line in zip(vectors, lines):
                tail = piece[pl.ds(height, tail_rows), pl.ds((p - 4) * rows, rows)]
                line[pl.ds(lax.axis_index("batch") ^ j, 1), :] = tail.astype(jnp.float32)[0:1]
        for line, out in zip(lines, outs[len(parts) - len(vectors) :]):
            out[...] = line[...].astype(out.dtype)
        for c in started:
            c.wait()

    shapes = [(replicas * rows, cols)] * 3 + [(cols, replicas * rows)] + [(replicas, rows)] * 2
    kinds = [jnp.bfloat16 if p < 4 or ends else jnp.float32 for p in parts]
    hbm = pl.BlockSpec(memory_space=pltpu.HBM)
    vmem = pl.BlockSpec(memory_space=pltpu.VMEM)
    spaces = [hbm if p < 4 else vmem for p in parts]
    outs = pl.pallas_call(
        kernel,
        out_shape=[jax.ShapeDtypeStruct(shapes[p], kind) for p, kind in zip(parts, kinds)],
        in_specs=[vmem] * (len(slabs) + 1) + (spaces if begun else []),
        out_specs=spaces,
        scratch_shapes=[pltpu.VMEM(x, jnp.float32) for x in lines_out] + [pltpu.SemaphoreType.DMA((1,))],
        input_output_aliases={len(slabs) + 1 + i: i for i, p in enumerate(parts) if p < 4} if begun else {},
        name="unpack",
        compiler_params=pltpu.CompilerParams(vmem_limit_bytes=vmem_grant),
    )(*[pieces[j] for j in slabs], tick, *begun)
    return [x if p < 4 or not ends else x.reshape(-1) for p, x in zip(parts, outs)]


def unpack_plain(pieces, rows, cols, replicas):
    here = lax.axis_index("batch")
    stacked = jnp.stack(pieces)
    ordered = stacked[jnp.arange(replicas) ^ here]
    full = [ordered[:, i * rows : (i + 1) * rows].reshape(replicas * rows, cols) for i in range(3)]
    mixed = ordered[:, 3 * rows : 4 * rows].reshape(replicas, cols, rows)
    full.append(mixed.transpose(1, 0, 2).reshape(cols, replicas * rows))
    tail = ordered[:, 4 * rows]
    return (*full, tail[:, :rows].reshape(-1), tail[:, rows : 2 * rows].reshape(-1))


order_of_8 = (
    ((0, 7, 0),), ((0, 5, 0),), ((0, 7, 1),), ((0, 3, 0),), ((0, 6, 0),), ((0, 6, 1),), ((0, 5, 1),),
    ((0, 3, 1),), ((0, 1, 0),), ((0, 4, 0),), ((0, 2, 0),), ((0, 4, 1),), ((0, 2, 1),), ((0, 1, 1),),
    ((1, 4, 0),), ((1, 2, 0),), ((1, 1, 0),), ((1, 1, 1),), ((1, 4, 1),), ((1, 3, 0),), ((1, 2, 1),),
    ((1, 5, 0),), ((1, 6, 1),), ((1, 5, 1),), ((1, 6, 0),), ((1, 3, 1),), ((1, 7, 0),), ((1, 7, 1),),
)
bits_of_8 = {(0, 7, 1): 2, (1, 7, 0): 2}
packs_of_8 = ((7, 5, 3), (6, 1, 4, 2, 0))


def plan_of(replicas, fits):
    groups = groups_of(fits)
    every = [(w, j, g) for w in range(2) for j in range(1, replicas) for g in range(len(groups))]
    bits = {at: at[1] & -at[1] for at in every}
    if fits and replicas == 8:
        bits.update(bits_of_8)
        return groups, bits, list(order_of_8)
    chunks = [*range(replicas - 1, 0, -2), *range(replicas - 2, 0, -2)]
    back = sorted(range(1, replicas), key=lambda j: (j & 1, j.bit_count(), j))
    order = [((w, j, g),) for w, js in ((0, chunks), (1, back)) for j in js for g in range(len(groups))]
    return groups, bits, order


def inputs_of(at, bits):
    w, j, g = at
    if w == 0:
        return [k for k in bits if k[0] == 0 and k[2] == g and k[1] ^ bits[k] == j]
    if j != bits[at]:
        return [(1, j ^ bits[at], g)]
    return [k for k in bits if k[0] == 0 and k[2] == g and k[1] == bits[k]]


def ticks_of(bits, order):
    late, seen = {}, set()
    home = {at: exchange for exchange in order for at in exchange}
    for before, exchange in zip(order, order[1:]):
        new = []
        for at in exchange:
            new += [home[k] for k in inputs_of(at, bits) if home[k] not in seen and home[k] not in new]
        seen.update(new)
        new = [k for k in new if k != before]
        if new:
            late[before] = new
    return late


def replica_step(*arrays):
    partials = tuple(a[0] for a in arrays[:6])
    masters = arrays[6:]
    replicas = lax.axis_size("batch")
    here = lax.axis_index("batch")
    rows, cols, fits = sizes_of(partials[0], partials[3], replicas)
    scale = 2.0 ** math.floor(math.log2(65504.0 / (largest_partial * replicas)))
    groups, bits, order = plan_of(replicas, fits)
    every = range(replicas)
    calls = packs_of_8 if fits and replicas == 8 else (tuple(every),)

    if fits:
        slabs = {}
        for chunks in calls:
            slabs.update(zip(chunks, pack_tiles(partials, chunks, replicas)))
    else:
        slabs = dict(zip(every, pack_plain(partials, [here ^ j for j in every], replicas, here)))

    def swap(xs, exchange):
        (bit,) = {bits[at] for at in exchange}
        x = xs[0] if len(xs) == 1 else jnp.concatenate(xs)
        x = lax.ppermute(x, "batch", [(i, i ^ bit) for i in every])
        ends = [sum(y.shape[0] for y in xs[: i + 1]) for i in range(len(xs))]
        return [x] if len(xs) == 1 else [x[end - y.shape[0] : end] for end, y in zip(ends, xs)]

    tall = slabs[0].shape[0]
    bounds = []
    for g, parts in enumerate(groups):
        first = rows * sum(p < 4 for q in groups[:g] for p in q)
        bounds.append((first, tall if 4 in parts else first + rows * len(parts)))
    got = {(j, g): [] for j in slabs for g in range(len(groups))}
    ahead = None

    def total(j, g):
        nonlocal ahead
        low, high = bounds[g]
        mine = slabs[j][low:high] * scale
        if not got[j, g]:
            return mine
        if ahead is not None:
            got[j, g][0], ahead = lax.optimization_barrier((got[j, g][0], ahead))
        return sum((x.astype(jnp.float32) for x in got[j, g]), mine)

    rate = learn_rate * replicas**-0.5 / scale
    ticks = ticks_of(bits, order) if fits else {}
    tick = masters[4][None]
    own, full, pieces = [None] * 6, [None] * 6, {}
    for exchange in order:
        sends = []
        for w, j, g in exchange:
            if w == 0:
                sends.append(total(j, g).astype(jnp.float16))
                if got[j, g]:
                    ahead = sends[-1]
                continue
            if (0, g) not in pieces:
                ahead = total(0, g)
                step = step_tiles if fits else step_plain
                pieces[0, g], new = step(ahead, masters, groups[g], rate, rows, cols)
                for p, x in zip(groups[g], new):
                    own[p] = x
            sends.append(pieces[j ^ bits[w, j, g], g])
        for (w, j, g), x in zip(exchange, swap(sends, exchange)):
            if w == 0:
                got[j ^ bits[w, j, g], g].append(x)
            else:
                pieces[j, g] = x
        if exchange in ticks:
            tick = lax.optimization_barrier(tick) + 1.0
    for g, parts in enumerate(groups):
        mine = {j: pieces[j, g] for j in range(replicas)}
        if not fits:
            done = unpack_plain([mine[j] for j in range(replicas)], rows, cols, replicas)
        elif g == order[-1][-1][2]:
            last = [at[1] for exchange in order for at in exchange if at[0] == 1 and at[2] == g][-2:]
            last = {j: mine.pop(j) for j in last}
            done = unpack_tiles(mine, [], tick, parts, rows, cols, replicas)
            done = unpack_tiles(last, done, tick, parts, rows, cols, replicas)
        else:
            done = unpack_tiles(mine, [], tick, parts, rows, cols, replicas)
        for p, x in zip(parts, done):
            full[p] = x
    return (*full, *own)


def solution(mesh):
    in_specs = (
        P("batch", None, "cols"),
        P("batch", None, "cols"),
        P("batch", None, "cols"),
        P("batch", "cols", None),
        P("batch", None),
        P("batch", None),
        P("batch", "cols"),
        P("batch", "cols"),
        P("batch", "cols"),
        P("cols", "batch"),
        P("batch"),
        P("batch"),
    )
    out_specs = (
        P(None, "cols"),
        P(None, "cols"),
        P(None, "cols"),
        P("cols", None),
        P(),
        P(),
        P("batch", "cols"),
        P("batch", "cols"),
        P("batch", "cols"),
        P("cols", "batch"),
        P("batch"),
        P("batch"),
    )
    return jax.shard_map(replica_step, mesh=mesh, in_specs=in_specs, out_specs=out_specs, check_vma=False)
```
